32 devices in a mesh: gz: 32 (over z, y, x, core).
Axes of the slice: x: 2, y: 2, z: 4, core: 2. Of those that a mesh axis runs over, the one named last changes fastest.
Arguments:
- state: float32 [8, 32, 64, 256], P(None, 'gz'), may hold values from -18 to 18
- explicit_rhs: float32 [2, 8, 32, 64, 256], P(None, None, 'gz'), may hold values from -6 to 6
- implicit_rhs: float32 [2, 8, 32, 64, 256], P(None, None, 'gz'), may hold values from -6 to 6
- implicit_coef: float32 [8], replicated, may hold values from 0.5 to 4
Outputs:
- section_value: float32 [8, 32, 64, 256], P(None, 'gz')
- weighted_rms: float32 [], replicated
The draws below stay inside these ranges and needn't reach their ends.
All inputs are finite; a program needn't handle non-finite values.
Results may differ from the reference program's by a relative error of at most 0.0001.
Values sent between devices are 32-bit elements; how exact they have to be, the bound alone decides.
No kernel may reach another device: no remote copies, remote signals or barrier semaphores. Data moves between devices by JAX's collectives and lax.ppermute only.
A program may use at most 64 MiB of HBM per device.

```python
import math
import jax
import jax.numpy as jnp
from jax import lax

S = 8
NY = 64
NX = 256
ITERS = 3
NZ = 32


def draw_state(key, part):
    depth = jnp.arange(NZ, dtype=jnp.float32) / NZ
    amplitude = (1.0 + 2.0 * depth)[None, :, None, None]
    noise = jnp.clip(jax.random.normal(key, (S, NZ, NY, NX), jnp.float32), -6.0, 6.0)
    return noise * amplitude


def shard_levels(own_key, dims, shards, smallest, high):
    factor_of = 1.0
    for position, shards_of in shards:
        steps = jax.random.uniform(jax.random.fold_in(jax.random.fold_in(own_key, 6), position), (shards_of,), jnp.float32, smallest / len(shards), high / len(shards))
        factor_of = factor_of * jnp.repeat(jnp.exp(steps), dims[position] // shards_of).reshape((-1,) + (1,) * (len(dims) - 1 - position))
    return factor_of


def scatter_about(key, extent, width, most, cuts=(), kind=jnp.bfloat16):
    factor_of = shard_levels(key, extent, cuts, -0.22, 0.18) if cuts else 1.0
    values = jax.random.normal(key, extent, jnp.float32) * width * factor_of
    return jnp.minimum(jnp.maximum(values, -most), most).astype(kind)


def setup_inputs(seed: int = 0) -> dict:
    keys = jax.random.split(jax.random.key(seed), 5)
    state = draw_state(jax.random.fold_in(keys[4], 71), 0)
    explicit_rhs = scatter_about(keys[1], (2, S, NZ, NY, NX), 1.0, 6.0, ((2, 32),), jnp.float32)
    implicit_rhs = scatter_about(keys[2], (2, S, NZ, NY, NX), 1.0, 6.0, ((2, 32),), jnp.float32)
    implicit_coef = jnp.clip(jnp.exp(jax.random.uniform(keys[3], (S,), jnp.float32, math.log(0.5), math.log(4.0))), 0.5, 4.0)
    return dict(state=state, explicit_rhs=explicit_rhs, implicit_rhs=implicit_rhs, implicit_coef=implicit_coef)


explicit_weights = (5535828885825.0 / 10492691773637.0, 788022342437.0 / 10882634858940.0)
implicit_weights = (2746238789719.0 / 10658868560708.0, -640167445237.0 / 6845629431997.0)

def operate(field, implicit_coef):
    flat = jnp.pad(field, ((0, 0), (0, 0), (1, 1), (1, 1)))
    beside = jnp.roll(field, 1, axis=1) + jnp.roll(field, -1, axis=1)
    beside = beside + flat[:, :, 2:, 1:-1] + flat[:, :, :-2, 1:-1] + flat[:, :, 1:-1, 2:] + flat[:, :, 1:-1, :-2]
    return field - implicit_coef[:, None, None, None] * (beside - 6.0 * field)

def species_sum(first, second):
    return lax.optimization_barrier(jnp.sum(first * second, axis=(1, 2, 3)))

def widen(values):
    return values[:, None, None, None]

def reference(state, explicit_rhs, implicit_rhs, implicit_coef):
    section_in = state + explicit_weights[0] * explicit_rhs[0] + explicit_weights[1] * explicit_rhs[1]
    section_in = section_in + implicit_weights[0] * implicit_rhs[0] + implicit_weights[1] * implicit_rhs[1]
    solution = section_in
    residual = section_in - operate(section_in, implicit_coef)
    direction = residual
    norm_now = species_sum(residual, residual)
    for iteration in range(ITERS):
        image = operate(direction, implicit_coef)
        step_size = norm_now / species_sum(direction, image)
        solution = solution + widen(step_size) * direction
        residual = residual - widen(step_size) * image
        if iteration + 1 < ITERS:
            norm_next = species_sum(residual, residual)
            direction = residual + widen(norm_next / norm_now) * direction
            norm_now = norm_next
    scaled = (solution - section_in) / (1.0 + 0.1 * jnp.abs(state))
    weighted_rms = jnp.sqrt(jnp.sum(scaled * scaled) / (S * NZ * NY * NX))
    return (solution, weighted_rms)
```

```python
import jax
import jax.numpy as jnp
from jax import lax
from jax.experimental import pallas as pl
from jax.experimental.pallas import tpu as pltpu
from jax.sharding import PartitionSpec as P

explicit_weights = (5535828885825.0 / 10492691773637.0, 788022342437.0 / 10882634858940.0)
implicit_weights = (2746238789719.0 / 10658868560708.0, -640167445237.0 / 6845629431997.0)

STRIDE = 8


def beside_plane(field):
    rows, cols = field.shape
    row = lax.broadcasted_iota(jnp.int32, field.shape, 0)
    col = lax.broadcasted_iota(jnp.int32, field.shape, 1)
    left = jnp.where(col == 0, 0.0, pltpu.roll(field, 1, 1))
    right = jnp.where(col == cols - 1, 0.0, pltpu.roll(field, cols - 1, 1))
    up = jnp.where(row == 0, 0.0, pltpu.roll(field, 1, 0))
    down = jnp.where(row == rows - 1, 0.0, pltpu.roll(field, rows - 1, 0))
    return (left + right) + (up + down)


def folded(values):
    rows, cols = values.shape
    total = None
    for r in range(0, rows, 8):
        for c in range(0, cols, 128):
            piece = values[r : r + 8, c : c + 128]
            total = piece if total is None else total + piece
    return total


def moments_kernel(own, low, high, low2, high2, far, state, basis, sums, g0, g1, g2, rows):
    half = own.shape[1]
    rows[...] = jnp.zeros(rows.shape, jnp.float32)
    sixth = 1.0 / 6.0

    def species(s, carry):
        def plane(z):
            if z == -3:
                return low2[0, s]
            if z < 0:
                return low[z + 2, s]
            if z < 2:
                return own[z, s]
            if z < 4:
                return high[z - 2, s]
            return high2[0, s]

        for z in range(-3, 5):
            value = plane(z)
            total = beside_plane(value) - 6.0 * value
            if z > -3:
                total = total + plane(z - 1)
            if z < 4:
                total = total + plane(z + 1)
            g0[z + 3] = total
        for z in range(-2, 4):
            value = g0[z + 3]
            g1[z + 2] = (beside_plane(value) + (g0[z + 2] + g0[z + 4])) * sixth
        moments = [None] * 12
        across = None

        def put(k, value):
            value = folded(value)
            moments[k] = value if moments[k] is None else moments[k] + value

        for z in range(-1, 3):
            value = g1[z + 2]
            g2[z + 1] = (beside_plane(value) + (g1[z + 1] + g1[z + 3])) * sixth
        third = 1.0 / 3.0
        for z in range(2):
            a, b, c = g0[z + 3], g1[z + 2], g2[z + 1]
            basis[0, z, s] = a
            basis[1, z, s] = b
            basis[2, z, s] = c
            put(0, a * a)
            put(1, a * b)
            put(2, b * b)
            put(3, b * c)
            put(4, c * c)
            put(5, c * (beside_plane(c) * sixth + third * g2[z + 2]))
            weight = 1.0 / (1.0 + 0.1 * jnp.abs(state[z, s]))
            a, b, c = a * weight, b * weight, c * weight
            put(6, a * a)
            put(7, a * b)
            put(8, a * c)
            put(9, b * b)
            put(10, b * c)
            put(11, c * c)
        reach = third / 36.0
        put(5, reach * (plane(3) * g2[0] + (1.0 / 36.0) * (far[0, s] * plane(-1))))
        for k in range(12):
            rows[pl.ds(k * STRIDE + s, 1), :] = jnp.sum(moments[k], axis=0, keepdims=True)
        return carry

    lax.fori_loop(0, half, species, 0)
    summed = jnp.sum(jnp.transpose(rows[...]), axis=0, keepdims=True)
    sums[...] = jnp.broadcast_to(summed, sums.shape)


def steps_kernel(parts, coef, own, basis, kept, sent, rms, *, cells):
    devices = parts.shape[0]
    half = own.shape[1]
    mine = lax.axis_index("gz") % 2
    total = parts[0:8, :]
    for d in range(8, devices, 8):
        total = total + parts[d : d + 8, :]
    total = total + pltpu.roll(total, 2, 0)
    total = total + pltpu.roll(total, 4, 0)
    m = [total if k == 0 else pltpu.roll(total, 128 - k * STRIDE, 1) for k in range(12)]
    six_c = 6.0 * coef[...]
    c = coef[...]
    diag = 1.0 + six_c
    smallest = 1.0 / (1.0 + 2.0 * six_c)

    def inner(p, q, shift):
        result = None
        for i, pi in enumerate(p):
            for j, qj in enumerate(q):
                term = pi * qj * m[i + j + shift]
                result = term if result is None else result + term
        return result

    def times(p):
        zero = jnp.zeros_like(c)
        return [diag * a - six_c * b for a, b in zip(list(p) + [zero], [zero] + list(p))]

    residual = [jnp.ones_like(c)]
    direction = list(residual)
    norm_now = m[0]
    answer = [jnp.zeros_like(c)] * 3
    for iteration in range(3):
        energy = diag * inner(direction, direction, 0) - six_c * inner(direction, direction, 1)
        step = jnp.minimum(jnp.maximum(norm_now / energy, smallest), 1.0)
        answer = [a + step * d for a, d in zip(answer, direction + [jnp.zeros_like(c)] * 3)]
        if iteration + 1 < 3:
            image = times(direction)
            residual = [a - step * b for a, b in zip(residual + [jnp.zeros_like(c)], image)]
            norm_next = jnp.maximum(inner(residual, residual, 0), 0.0)
            beta = norm_next / norm_now
            direction = [a + beta * b for a, b in zip(residual, direction + [jnp.zeros_like(c)])]
            norm_now = norm_next
    answer = [c * a for a in answer]
    y0, y1, y2 = answer
    error = (
        y0 * y0 * m[6]
        + y1 * y1 * m[9]
        + y2 * y2 * m[11]
        + 2.0 * (y0 * y1 * m[7] + y0 * y2 * m[8] + y1 * y2 * m[10])
    )
    row = lax.broadcasted_iota(jnp.int32, c.shape, 0)
    col = lax.broadcasted_iota(jnp.int32, c.shape, 1)
    error = jnp.sum(jnp.where((row < 2) & (col < half), error, 0.0), keepdims=True)
    rms[...] = jnp.sqrt(jnp.maximum(error, 0.0) * (1.0 / cells))
    for s in range(half):
        chosen = (row == mine) & (col == s)
        w = [jnp.sum(jnp.where(chosen, y, 0.0)) for y in answer]
        for z, out in ((mine, kept), (1 - mine, sent)):
            out[s] = own[z, s] + (
                w[0] * basis[0, z, s] + (w[1] * basis[1, z, s] + w[2] * basis[2, z, s])
            )


def shards(state, explicit_rhs, implicit_rhs, implicit_coef):
    count = lax.axis_size("gz")
    species, planes, ny, nx = state.shape
    half = species // 2
    assert planes == 1 and species % 2 == 0 and count % 8 == 0 and half <= STRIDE
    vmem = pl.BlockSpec(memory_space=pltpu.VMEM)

    def move(value, shift):
        return lax.ppermute(value, "gz", [(i, (i + shift) % count) for i in range(count)])

    def swap(value):
        return lax.ppermute(value, "gz", [(i, i ^ 1) for i in range(count)])

    section_in = (
        state + explicit_weights[0] * explicit_rhs[0] + explicit_weights[1] * explicit_rhs[1]
    )
    section_in = (
        section_in + implicit_weights[0] * implicit_rhs[0] + implicit_weights[1] * implicit_rhs[1]
    )
    section_in = section_in[:, 0]
    odd = lax.axis_index("gz") % 2

    def paired(field):
        keep = jnp.where(odd == 0, field[:half], field[half:])
        give = jnp.where(odd == 0, field[half:], field[:half])
        take = swap(give)
        return jnp.stack([jnp.where(odd == 0, keep, take), jnp.where(odd == 0, take, keep)])

    own = paired(section_in)
    low = move(own, 2)
    high = move(own, -2)
    low2 = move(own[1:], 4)
    high2 = move(own[:1], -4)
    far = move(own[:1], 8)
    weight_state = paired(state[:, 0])
    basis, sums = pl.pallas_call(
        moments_kernel,
        in_specs=[vmem] * 7,
        out_specs=[vmem] * 2,
        out_shape=[
            jax.ShapeDtypeStruct((3,) + own.shape, jnp.float32),
            jax.ShapeDtypeStruct((count, 128), jnp.float32),
        ],
        scratch_shapes=[
            pltpu.VMEM((8, ny, nx), jnp.float32),
            pltpu.VMEM((6, ny, nx), jnp.float32),
            pltpu.VMEM((4, ny, nx), jnp.float32),
            pltpu.VMEM((128, 128), jnp.float32),
        ],
        name="moments",
    )(own, low, high, low2, high2, far, weight_state)
    parts = lax.all_to_all(sums, "gz", 0, 0)
    coef = jnp.tile(jnp.pad(implicit_coef.reshape(2, half), ((0, 0), (0, 128 - half)), constant_values=1.0), (4, 1))
    cells = species * count * ny * nx
    kept, sent, rms = pl.pallas_call(
        lambda *refs: steps_kernel(*refs, cells=cells),
        in_specs=[vmem] * 4,
        out_specs=[vmem] * 3,
        out_shape=[
            jax.ShapeDtypeStruct((half, ny, nx), jnp.float32),
            jax.ShapeDtypeStruct((half, ny, nx), jnp.float32),
            jax.ShapeDtypeStruct((1, 1), jnp.float32),
        ],
        name="steps",
    )(parts, coef, own, basis)
    taken = swap(sent)
    solution = jnp.concatenate(
        [jnp.where(odd == 0, kept, taken), jnp.where(odd == 0, taken, kept)]
    )
    return (solution[:, None], rms[0, 0])


def solution(mesh):
    placed = (
        P(None, "gz", None, None),
        P(None, None, "gz", None, None),
        P(None, None, "gz", None, None),
        P(),
    )
    return jax.shard_map(
        shards,
        mesh=mesh,
        in_specs=placed,
        out_specs=(P(None, "gz", None, None), P()),
        check_vma=False,
    )
```

```python
import jax
import jax.numpy as jnp
from jax import lax
from jax.experimental import pallas as pl
from jax.experimental.pallas import tpu as pltpu
from jax.sharding import PartitionSpec as P


explicit_weights = (5535828885825.0 / 10492691773637.0, 788022342437.0 / 10882634858940.0)
implicit_weights = (2746238789719.0 / 10658868560708.0, -640167445237.0 / 6845629431997.0)

STRIDE = 8


def beside_plane(field):
    rows, cols = field.shape
    row = lax.broadcasted_iota(jnp.int32, field.shape, 0)
    col = lax.broadcasted_iota(jnp.int32, field.shape, 1)
    left = jnp.where(col == 0, 0.0, pltpu.roll(field, 1, 1))
    right = jnp.where(col == cols - 1, 0.0, pltpu.roll(field, cols - 1, 1))
    up = jnp.where(row == 0, 0.0, pltpu.roll(field, 1, 0))
    down = jnp.where(row == rows - 1, 0.0, pltpu.roll(field, rows - 1, 0))
    return (left + right) + (up + down)


def folded(values):
    rows, cols = values.shape
    total = None
    for r in range(0, rows, 8):
        for c in range(0, cols, 128):
            piece = values[r : r + 8, c : c + 128]
            total = piece if total is None else total + piece
    return total


def moments_kernel(own, low, high, low2, high2, far, state, basis, sums, g0, g1, g2, rows):
    half = own.shape[1]
    rows[...] = jnp.zeros(rows.shape, jnp.float32)
    sixth = 1.0 / 6.0

    def species(s, carry):
        def plane(z):
            if z == -3:
                return low2[s]
            if z < 0:
                return low[z + 2, s]
            if z < 2:
                return own[z, s]
            if z < 4:
                return high[z - 2, s]
            return high2[s]

        for z in range(-3, 5):
            value = plane(z)
            total = beside_plane(value) - 6.0 * value
            if z > -3:
                total = total + plane(z - 1)
            if z < 4:
                total = total + plane(z + 1)
            g0[z + 3] = total
        for z in range(-2, 4):
            value = g0[z + 3]
            g1[z + 2] = (beside_plane(value) + (g0[z + 2] + g0[z + 4])) * sixth
        moments = [None] * 12

        def put(k, value):
            value = folded(value)
            moments[k] = value if moments[k] is None else moments[k] + value

        for z in range(-1, 3):
            value = g1[z + 2]
            g2[z + 1] = (beside_plane(value) + (g1[z + 1] + g1[z + 3])) * sixth
        third = 1.0 / 3.0
        for z in range(2):
            a, b, c = g0[z + 3], g1[z + 2], g2[z + 1]
            basis[0, z, s] = a
            basis[1, z, s] = b
            basis[2, z, s] = c
            put(0, a * a)
            put(1, a * b)
            put(2, b * b)
            put(3, b * c)
            put(4, c * c)
            put(5, c * (beside_plane(c) * sixth + third * g2[z + 2]))
            weight = 1.0 / (1.0 + 0.1 * jnp.abs(state[z, s]))
            a, b, c = a * weight, b * weight, c * weight
            put(6, a * a)
            put(7, a * b)
            put(8, a * c)
            put(9, b * b)
            put(10, b * c)
            put(11, c * c)
        reach = third / 36.0
        put(5, reach * (plane(3) * g2[0] + (1.0 / 36.0) * (far[s] * plane(-1))))
        for k in range(12):
            rows[pl.ds(k * STRIDE + s, 1), :] = jnp.sum(moments[k], axis=0, keepdims=True)
        return carry

    lax.fori_loop(0, half, species, 0)
    summed = jnp.sum(jnp.transpose(rows[...]), axis=0, keepdims=True)
    sums[...] = jnp.broadcast_to(summed, sums.shape)


def steps_kernel(parts, coef, own, basis, kept, sent, rms, *, cells):
    devices = parts.shape[0]
    half = own.shape[1]
    mine = lax.axis_index("gz") % 2
    total = parts[0:8, :]
    for d in range(8, devices, 8):
        total = total + parts[d : d + 8, :]
    total = total + pltpu.roll(total, 2, 0)
    total = total + pltpu.roll(total, 4, 0)
    m = [total if k == 0 else pltpu.roll(total, 128 - k * STRIDE, 1) for k in range(12)]
    six_c = 6.0 * coef[...]
    c = coef[...]
    diag = 1.0 + six_c
    smallest = 1.0 / (1.0 + 2.0 * six_c)

    def inner(p, q, shift):
        result = None
        for i, pi in enumerate(p):
            for j, qj in enumerate(q):
                term = pi * qj * m[i + j + shift]
                result = term if result is None else result + term
        return result

    def times(p):
        zero = jnp.zeros_like(c)
        return [diag * a - six_c * b for a, b in zip(list(p) + [zero], [zero] + list(p))]

    residual = [jnp.ones_like(c)]
    direction = list(residual)
    norm_now = m[0]
    answer = [jnp.zeros_like(c)] * 3
    for iteration in range(3):
        energy = diag * inner(direction, direction, 0) - six_c * inner(direction, direction, 1)
        step = jnp.minimum(jnp.maximum(norm_now / energy, smallest), 1.0)
        answer = [a + step * d for a, d in zip(answer, direction + [jnp.zeros_like(c)] * 3)]
        if iteration + 1 < 3:
            image = times(direction)
            residual = [a - step * b for a, b in zip(residual + [jnp.zeros_like(c)], image)]
            norm_next = jnp.maximum(inner(residual, residual, 0), 0.0)
            beta = norm_next / norm_now
            direction = [a + beta * b for a, b in zip(residual, direction + [jnp.zeros_like(c)])]
            norm_now = norm_next
    answer = [c * a for a in answer]
    y0, y1, y2 = answer
    error = (
        y0 * y0 * m[6]
        + y1 * y1 * m[9]
        + y2 * y2 * m[11]
        + 2.0 * (y0 * y1 * m[7] + y0 * y2 * m[8] + y1 * y2 * m[10])
    )
    row = lax.broadcasted_iota(jnp.int32, c.shape, 0)
    col = lax.broadcasted_iota(jnp.int32, c.shape, 1)
    error = jnp.sum(jnp.where((row < 2) & (col < half), error, 0.0), keepdims=True)
    rms[...] = jnp.sqrt(jnp.maximum(error, 0.0) * (1.0 / cells))
    for s in range(half):
        chosen = (row == mine) & (col == s)
        w = [jnp.sum(jnp.where(chosen, y, 0.0)) for y in answer]
        for z, out in ((mine, kept), (1 - mine, sent)):
            out[s] = own[z, s] + (
                w[0] * basis[0, z, s] + (w[1] * basis[1, z, s] + w[2] * basis[2, z, s])
            )


def section(state, explicit_rhs, implicit_rhs, implicit_coef):
    count = lax.axis_size("gz")
    species, planes, ny, nx = state.shape
    half = species // 2
    assert planes == 1 and species % 2 == 0 and count % 8 == 0 and half <= STRIDE
    vmem = pl.BlockSpec(memory_space=pltpu.VMEM)
    params = pltpu.CompilerParams(vmem_limit_bytes=24 << 20)
    device = lax.axis_index("gz")
    odd = device % 2 == 1
    chip_odd = device // 2 % 2 == 1
    chip_upper = device // 4 % 2 == 1

    def exchange(value, partner):
        pairs = [(i, partner(i // 2) % (count // 2) * 2 + i % 2) for i in range(count)]
        return lax.ppermute(value, "gz", pairs)

    def swap(value):
        return lax.ppermute(value, "gz", [(i, i ^ 1) for i in range(count)])

    section_in = (
        state + explicit_weights[0] * explicit_rhs[0] + explicit_weights[1] * explicit_rhs[1]
    )
    section_in = (
        section_in + implicit_weights[0] * implicit_rhs[0] + implicit_weights[1] * implicit_rhs[1]
    )
    section_in = section_in[:, 0]

    def paired(field):
        keep = jnp.where(odd, field[half:], field[:half])
        give = jnp.where(odd, field[:half], field[half:])
        take = swap(give)
        return jnp.where(odd, take, keep), jnp.where(odd, keep, take)

    even_plane, odd_plane = paired(section_in)
    own = jnp.stack([even_plane, odd_plane])
    by_x = exchange(own, lambda c: c ^ 1)
    by_y = exchange(jnp.where(chip_upper, even_plane, odd_plane), lambda c: c ^ 2)
    by_z = exchange(
        jnp.where(chip_upper, odd_plane, even_plane), lambda c: c + 2 if c // 2 % 2 else c - 2
    )
    far = exchange(even_plane, lambda c: c + 4)
    by_corner = exchange(own, lambda c: c + 1 if c % 2 else c - 1)
    low = jnp.where(chip_odd, by_x, by_corner)
    high = jnp.where(chip_odd, by_corner, by_x)
    low2 = jnp.where(chip_upper, by_y, by_z)
    high2 = jnp.where(chip_upper, by_z, by_y)
    weight_state = jnp.stack(paired(state[:, 0]))
    basis, sums = pl.pallas_call(
        moments_kernel,
        in_specs=[vmem] * 7,
        compiler_params=params,
        out_specs=[vmem] * 2,
        out_shape=[
            jax.ShapeDtypeStruct((3,) + own.shape, jnp.float32),
            jax.ShapeDtypeStruct((count, 128), jnp.float32),
        ],
        scratch_shapes=[
            pltpu.VMEM((8, ny, nx), jnp.float32),
            pltpu.VMEM((6, ny, nx), jnp.float32),
            pltpu.VMEM((4, ny, nx), jnp.float32),
            pltpu.VMEM((128, 128), jnp.float32),
        ],
        name="moments",
    )(own, low, high, low2, high2, far, weight_state)
    parts = lax.all_to_all(sums, "gz", 0, 0)
    coef = jnp.tile(jnp.pad(implicit_coef.reshape(2, half), ((0, 0), (0, 128 - half)), constant_values=1.0), (4, 1))
    cells = species * count * ny * nx
    kept, sent, rms = pl.pallas_call(
        lambda *refs: steps_kernel(*refs, cells=cells),
        in_specs=[vmem] * 4,
        compiler_params=params,
        out_specs=[vmem] * 3,
        out_shape=[
            jax.ShapeDtypeStruct((half, ny, nx), jnp.float32),
            jax.ShapeDtypeStruct((half, ny, nx), jnp.float32),
            jax.ShapeDtypeStruct((1, 1), jnp.float32),
        ],
        name="steps",
    )(parts, coef, own, basis)
    taken = swap(sent)
    solution = jnp.concatenate(
        [jnp.where(odd, taken, kept), jnp.where(odd, kept, taken)]
    )
    return (solution[:, None], rms[0, 0])


def solution(mesh):
    placed = (
        P(None, "gz", None, None),
        P(None, None, "gz", None, None),
        P(None, None, "gz", None, None),
        P(),
    )
    return jax.shard_map(
        section,
        mesh=mesh,
        in_specs=placed,
        out_specs=(P(None, "gz", None, None), P()),
        check_vma=False,
    )
```

```python
import jax
import jax.numpy as jnp
from jax import lax
from jax.experimental import pallas as pl
from jax.experimental.pallas import tpu as pltpu
from jax.sharding import PartitionSpec as P


explicit_weights = (5535828885825.0 / 10492691773637.0, 788022342437.0 / 10882634858940.0)
implicit_weights = (2746238789719.0 / 10658868560708.0, -640167445237.0 / 6845629431997.0)

STRIDE = 8


def beside_plane(field):
    rows, cols = field.shape
    row = lax.broadcasted_iota(jnp.int32, field.shape, 0)
    col = lax.broadcasted_iota(jnp.int32, field.shape, 1)
    left = jnp.where(col == 0, 0.0, pltpu.roll(field, 1, 1))
    right = jnp.where(col == cols - 1, 0.0, pltpu.roll(field, cols - 1, 1))
    up = jnp.where(row == 0, 0.0, pltpu.roll(field, 1, 0))
    down = jnp.where(row == rows - 1, 0.0, pltpu.roll(field, rows - 1, 0))
    return (left + right) + (up + down)


def folded(values):
    rows, cols = values.shape
    total = None
    for r in range(0, rows, 8):
        for c in range(0, cols, 128):
            piece = values[r : r + 8, c : c + 128]
            total = piece if total is None else total + piece
    return total


def moments_kernel(
    first, second, near_x, far_x, near_d, far_d, high2, low2, far, state, basis, sums, g0, g1, g2, rows
):
    half = first.shape[0]
    chip_odd = lax.axis_index("gz") // 2 % 2 == 1
    rows[...] = jnp.zeros(rows.shape, jnp.float32)
    window = (low2, far_d, near_d, first, second, near_x, far_x, high2)
    sixth = 1.0 / 6.0
    third = 1.0 / 3.0
    reach = 1.0 / 36.0

    def species(s, carry):
        def plane(z):
            return window[z + 3][s]

        for z in range(-3, 5):
            value = plane(z)
            total = beside_plane(value) - 6.0 * value
            if z > -3:
                total = total + plane(z - 1)
            if z < 4:
                total = total + plane(z + 1)
            g0[z + 3] = total
        for z in range(-2, 4):
            value = g0[z + 3]
            g1[z + 2] = (beside_plane(value) + (g0[z + 2] + g0[z + 4])) * sixth
        moments = [None] * 12

        def put(k, value):
            value = folded(value)
            moments[k] = value if moments[k] is None else moments[k] + value

        for z in range(-1, 3):
            value = g1[z + 2]
            g2[z + 1] = (beside_plane(value) + (g1[z + 1] + g1[z + 3])) * sixth
        for z in range(2):
            a, b, c = g0[z + 3], g1[z + 2], g2[z + 1]
            basis[0, z, s] = a
            basis[1, z, s] = b
            basis[2, z, s] = c
            put(0, a * a)
            put(1, a * b)
            put(2, b * b)
            put(3, b * c)
            put(4, c * c)
            put(5, sixth * (c * beside_plane(c)))
            weight = 1.0 / (1.0 + 0.1 * jnp.abs(state[z, s]))
            a, b, c = a * weight, b * weight, c * weight
            put(6, a * a)
            put(7, a * b)
            put(8, a * c)
            put(9, b * b)
            put(10, b * c)
            put(11, c * c)
        across = g2[1] * g2[2]
        across = across + 0.5 * (g2[3] * (g2[2] + reach * plane(-2)))
        across = across + 0.5 * (g2[0] * (g2[1] + reach * plane(3)))
        mate = jnp.where(chip_odd, plane(2), plane(-1))
        across = across + (reach * reach) * (far[s] * mate)
        put(5, third * across)
        for k in range(12):
            rows[pl.ds(k * STRIDE + s, 1), :] = jnp.sum(moments[k], axis=0, keepdims=True)
        return carry

    lax.fori_loop(0, half, species, 0)
    summed = jnp.sum(jnp.transpose(rows[...]), axis=0, keepdims=True)
    sums[...] = jnp.broadcast_to(summed, sums.shape)


def steps_kernel(parts, coef, first, second, basis, kept, sent, rms, *, cells):
    devices = parts.shape[0]
    half = first.shape[0]
    device = lax.axis_index("gz")
    core = device % 2
    mine = (device + device // 2) % 2
    total = parts[0:8, :]
    for d in range(8, devices, 8):
        total = total + parts[d : d + 8, :]
    total = total + pltpu.roll(total, 2, 0)
    total = total + pltpu.roll(total, 4, 0)
    m = [total if k == 0 else pltpu.roll(total, 128 - k * STRIDE, 1) for k in range(12)]
    six_c = 6.0 * coef[...]
    c = coef[...]
    diag = 1.0 + six_c
    smallest = 1.0 / (1.0 + 2.0 * six_c)

    def inner(p, q, shift):
        result = None
        for i, pi in enumerate(p):
            for j, qj in enumerate(q):
                term = pi * qj * m[i + j + shift]
                result = term if result is None else result + term
        return result

    def times(p):
        zero = jnp.zeros_like(c)
        return [diag * a - six_c * b for a, b in zip(list(p) + [zero], [zero] + list(p))]

    residual = [jnp.ones_like(c)]
    direction = list(residual)
    norm_now = m[0]
    answer = [jnp.zeros_like(c)] * 3
    for iteration in range(3):
        energy = diag * inner(direction, direction, 0) - six_c * inner(direction, direction, 1)
        step = jnp.minimum(jnp.maximum(norm_now / energy, smallest), 1.0)
        answer = [a + step * d for a, d in zip(answer, direction + [jnp.zeros_like(c)] * 3)]
        if iteration + 1 < 3:
            image = times(direction)
            residual = [a - step * b for a, b in zip(residual + [jnp.zeros_like(c)], image)]
            norm_next = jnp.maximum(inner(residual, residual, 0), 0.0)
            beta = norm_next / norm_now
            direction = [a + beta * b for a, b in zip(residual, direction + [jnp.zeros_like(c)])]
            norm_now = norm_next
    answer = [c * a for a in answer]
    y0, y1, y2 = answer
    error = (
        y0 * y0 * m[6]
        + y1 * y1 * m[9]
        + y2 * y2 * m[11]
        + 2.0 * (y0 * y1 * m[7] + y0 * y2 * m[8] + y1 * y2 * m[10])
    )
    row = lax.broadcasted_iota(jnp.int32, c.shape, 0)
    col = lax.broadcasted_iota(jnp.int32, c.shape, 1)
    error = jnp.sum(jnp.where((row < 2) & (col < half), error, 0.0), keepdims=True)
    rms[...] = jnp.sqrt(jnp.maximum(error, 0.0) * (1.0 / cells))
    for s in range(half):
        chosen = (row == core) & (col == s)
        w = [jnp.sum(jnp.where(chosen, y, 0.0)) for y in answer]
        for swapped, out in ((False, kept), (True, sent)):
            z = 1 - mine if swapped else mine
            start = jnp.where(z == 0, first[s], second[s])
            out[s] = start + (
                w[0] * basis[0, z, s] + (w[1] * basis[1, z, s] + w[2] * basis[2, z, s])
            )


def section(state, explicit_rhs, implicit_rhs, implicit_coef):
    count = lax.axis_size("gz")
    species, planes, ny, nx = state.shape
    half = species // 2
    assert planes == 1 and species % 2 == 0 and count % 8 == 0 and half <= STRIDE
    vmem = pl.BlockSpec(memory_space=pltpu.VMEM)
    params = pltpu.CompilerParams(vmem_limit_bytes=24 << 20)
    device = lax.axis_index("gz")
    odd = device % 2 == 1
    chip_odd = device // 2 % 2 == 1
    chip_upper = device // 4 % 2 == 1

    def exchange(value, partner):
        pairs = [(i, partner(i // 2) % (count // 2) * 2 + i % 2) for i in range(count)]
        return lax.ppermute(value, "gz", pairs)

    def swap(value):
        return lax.ppermute(value, "gz", [(i, i ^ 1) for i in range(count)])

    section_in = (
        state + explicit_weights[0] * explicit_rhs[0] + explicit_weights[1] * explicit_rhs[1]
    )
    section_in = (
        section_in + implicit_weights[0] * implicit_rhs[0] + implicit_weights[1] * implicit_rhs[1]
    )
    section_in = section_in[:, 0]

    mine = odd != chip_odd
    same = chip_odd == chip_upper

    def paired(field):
        keep = jnp.where(odd, field[half:], field[:half])
        give = jnp.where(odd, field[:half], field[half:])
        take = swap(give)
        return jnp.where(mine, take, keep), jnp.where(mine, keep, take)

    first, second = paired(section_in)
    near_x = exchange(second, lambda c: c ^ 1)
    by_y = exchange(jnp.where(same, second, first), lambda c: c ^ 2)
    by_z = exchange(jnp.where(same, first, second), lambda c: c + 2 if c // 2 % 2 else c - 2)
    far = exchange(jnp.where(chip_odd, second, first), lambda c: c + 4)
    far_x = exchange(first, lambda c: c ^ 1)
    far_d = exchange(near_x, lambda c: c - 2 if c % 2 else c + 2)
    high2 = jnp.where(same, by_y, by_z)
    low2 = jnp.where(same, by_z, by_y)
    near_d = exchange(high2, lambda c: c ^ 1)
    weight_state = jnp.stack(paired(state[:, 0]))
    basis, sums = pl.pallas_call(
        moments_kernel,
        in_specs=[vmem] * 10,
        compiler_params=params,
        out_specs=[vmem] * 2,
        out_shape=[
            jax.ShapeDtypeStruct((3, 2, half, ny, nx), jnp.float32),
            jax.ShapeDtypeStruct((count, 128), jnp.float32),
        ],
        scratch_shapes=[
            pltpu.VMEM((8, ny, nx), jnp.float32),
            pltpu.VMEM((6, ny, nx), jnp.float32),
            pltpu.VMEM((4, ny, nx), jnp.float32),
            pltpu.VMEM((128, 128), jnp.float32),
        ],
        name="moments",
    )(first, second, near_x, far_x, near_d, far_d, high2, low2, far, weight_state)
    parts = lax.all_to_all(sums, "gz", 0, 0)
    coef = jnp.tile(jnp.pad(implicit_coef.reshape(2, half), ((0, 0), (0, 128 - half)), constant_values=1.0), (4, 1))
    cells = species * count * ny * nx
    kept, sent, rms = pl.pallas_call(
        lambda *refs: steps_kernel(*refs, cells=cells),
        in_specs=[vmem] * 5,
        compiler_params=params,
        out_specs=[vmem] * 3,
        out_shape=[
            jax.ShapeDtypeStruct((half, ny, nx), jnp.float32),
            jax.ShapeDtypeStruct((half, ny, nx), jnp.float32),
            jax.ShapeDtypeStruct((1, 1), jnp.float32),
        ],
        name="steps",
    )(parts, coef, first, second, basis)
    taken = swap(sent)
    solution = jnp.concatenate(
        [jnp.where(odd, taken, kept), jnp.where(odd, kept, taken)]
    )
    return (solution[:, None], rms[0, 0])


def solution(mesh):
    placed = (
        P(None, "gz", None, None),
        P(None, None, "gz", None, None),
        P(None, None, "gz", None, None),
        P(),
    )
    return jax.shard_map(
        section,
        mesh=mesh,
        in_specs=placed,
        out_specs=(P(None, "gz", None, None), P()),
        check_vma=False,
    )
```

```python
import jax
import jax.numpy as jnp
from jax import lax
from jax.experimental import pallas as pl
from jax.experimental.pallas import tpu as pltpu
from jax.sharding import PartitionSpec as P


explicit_weights = (5535828885825.0 / 10492691773637.0, 788022342437.0 / 10882634858940.0)
implicit_weights = (2746238789719.0 / 10658868560708.0, -640167445237.0 / 6845629431997.0)

STRIDE = 8


def beside_plane(field):
    rows, cols = field.shape
    row = lax.broadcasted_iota(jnp.int32, field.shape, 0)
    col = lax.broadcasted_iota(jnp.int32, field.shape, 1)
    left = jnp.where(col == 0, 0.0, pltpu.roll(field, 1, 1))
    right = jnp.where(col == cols - 1, 0.0, pltpu.roll(field, cols - 1, 1))
    up = jnp.where(row == 0, 0.0, pltpu.roll(field, 1, 0))
    down = jnp.where(row == rows - 1, 0.0, pltpu.roll(field, rows - 1, 0))
    return (left + right) + (up + down)


def half_beside(field):
    row = lax.broadcasted_iota(jnp.int32, field.shape, 0)
    col = lax.broadcasted_iota(jnp.int32, field.shape, 1)
    left = jnp.where(col == 0, 0.0, pltpu.roll(field, 1, 1))
    up = jnp.where(row == 0, 0.0, pltpu.roll(field, 1, 0))
    return left + up


def folded(values):
    rows, cols = values.shape
    total = None
    for r in range(0, rows, 8):
        for c in range(0, cols, 128):
            piece = values[r : r + 8, c : c + 128]
            total = piece if total is None else total + piece
    return total


def upper_kernel(first, second, near_x, far_x, high2, low2, state, known, weight):
    half = first.shape[0]

    def species(s, carry):
        b0, b1, b2, b3, b4 = first[s], second[s], near_x[s], far_x[s], high2[s]
        known[2, s] = beside_plane(b0) - 6.0 * b0 + b1
        known[3, s] = beside_plane(low2[s]) - 6.0 * low2[s]
        a1 = beside_plane(b1) - 6.0 * b1 + (b0 + b2)
        known[0, s] = a1
        a2 = beside_plane(b2) - 6.0 * b2 + (b1 + b3)
        known[4, s] = beside_plane(a1) + a2
        a3 = beside_plane(b3) - 6.0 * b3 + (b2 + b4)
        c2 = beside_plane(a2) + (a1 + a3)
        known[1, s] = c2
        a4 = beside_plane(b4) - 6.0 * b4 + b3
        c3 = beside_plane(a3) + (a2 + a4)
        known[5, s] = beside_plane(c2) + c3
        for z in range(2):
            weight[z, s] = 1.0 / (1.0 + 0.1 * jnp.abs(state[z, s]))
        return carry

    lax.fori_loop(0, half, species, 0)


def moments_kernel(
    first, low2, near_x, far_x, near_d, far_d, far, known, weight, keep, give, sums, g0, g1, g2, rows
):
    half = first.shape[0]
    device = lax.axis_index("gz")
    mine = (device + device // 2) % 2
    rows[...] = jnp.zeros(rows.shape, jnp.float32)

    def species(s, carry):
        below, below2 = near_d[s], far_d[s]
        under0 = known[2, s] + below
        g0[0] = under0
        g0[1] = known[0, s]
        under1 = beside_plane(below) - 6.0 * below + (first[s] + below2)
        under2 = beside_plane(below2) - 6.0 * below2 + (below + low2[s])
        under3 = known[3, s] + below2
        c2 = beside_plane(under2) + (under1 + under3)
        c1 = beside_plane(under1) + (under0 + under2)
        g1[0] = beside_plane(under0) + (under1 + g0[1])
        g1[1] = known[4, s] + under0
        lower = beside_plane(c1) + (c2 + g1[0])
        g2[0] = beside_plane(g1[0]) + (c1 + g1[1])
        g2[1] = beside_plane(g1[1]) + (g1[0] + known[1, s])
        upper = known[5, s] + g1[1]
        moments = [None] * 12

        def put(k, value):
            value = folded(value)
            moments[k] = value if moments[k] is None else moments[k] + value

        for z in range(2):
            a, b, c = g0[z], g1[z], g2[z]
            put(0, a * a)
            put(1, a * b)
            put(2, b * b)
            put(3, b * c)
            put(4, c * c)
            put(5, c * half_beside(c))
            w = weight[z, s]
            a, b, c = a * w, b * w, c * w
            put(6, a * a)
            put(7, a * b)
            put(8, a * c)
            put(9, b * b)
            put(10, b * c)
            put(11, c * c)
        across = g2[0] * g2[1]
        across = across + 0.5 * (upper * (g2[1] + below2))
        across = across + 0.5 * (lower * (g2[0] + far_x[s]))
        across = across + far[s] * jnp.where(mine == 1, near_x[s], below)
        put(5, across)
        moments[5] = 2.0 * moments[5]
        for k, g in enumerate((g0, g1, g2)):
            keep[k, s] = g[mine]
            give[k, s] = g[1 - mine]
        for k in range(12):
            rows[pl.ds(k * STRIDE + s, 1), :] = jnp.sum(moments[k], axis=0, keepdims=True)
        return carry

    lax.fori_loop(0, half, species, 0)
    summed = jnp.sum(jnp.transpose(rows[...]), axis=0, keepdims=True)
    sums[...] = jnp.broadcast_to(summed[None], sums.shape)


def steps_kernel(parts, coef, kept, given, keep, take, out, rms, block, done, *, cells):
    half = kept.shape[0]
    core = lax.axis_index("gz") % 2
    devices = parts.shape[0]
    total = parts[0:8, 0, :]
    for d in range(8, devices, 8):
        total = total + parts[d : d + 8, 0, :]
    total = total + pltpu.roll(total, 2, 0)
    total = total + pltpu.roll(total, 4, 0)
    m = [total if k == 0 else pltpu.roll(total, 128 - k * STRIDE, 1) for k in range(12)]
    c = coef[...]
    diag = 1.0 + 6.0 * c
    smallest = 1.0 / (1.0 + 12.0 * c)

    def inner(p, q, shift):
        result = None
        for i, pi in enumerate(p):
            for j, qj in enumerate(q):
                term = pi * qj * m[i + j + shift]
                result = term if result is None else result + term
        return result

    def times(p):
        zero = jnp.zeros_like(c)
        return [diag * a - c * b for a, b in zip(list(p) + [zero], [zero] + list(p))]

    residual = [jnp.ones_like(c)]
    direction = list(residual)
    norm_now = m[0]
    answer = [jnp.zeros_like(c)] * 3
    for iteration in range(3):
        energy = diag * inner(direction, direction, 0) - c * inner(direction, direction, 1)
        step = jnp.minimum(jnp.maximum(norm_now / energy, smallest), 1.0)
        answer = [a + step * d for a, d in zip(answer, direction + [jnp.zeros_like(c)] * 3)]
        if iteration + 1 < 3:
            image = times(direction)
            residual = [a - step * b for a, b in zip(residual + [jnp.zeros_like(c)], image)]
            norm_next = jnp.maximum(inner(residual, residual, 0), 0.0)
            beta = norm_next / norm_now
            direction = [a + beta * b for a, b in zip(residual, direction + [jnp.zeros_like(c)])]
            norm_now = norm_next
    answer = [c * a for a in answer]
    y0, y1, y2 = answer
    error = (
        y0 * y0 * m[6]
        + y1 * y1 * m[9]
        + y2 * y2 * m[11]
        + 2.0 * (y0 * y1 * m[7] + y0 * y2 * m[8] + y1 * y2 * m[10])
    )
    row = lax.broadcasted_iota(jnp.int32, c.shape, 0)
    col = lax.broadcasted_iota(jnp.int32, c.shape, 1)
    error = jnp.sum(jnp.where((row < 2) & (col < half), error, 0.0), keepdims=True)
    rms[...] = jnp.sqrt(jnp.maximum(error, 0.0) * (1.0 / cells))
    copies = []
    for part, start, basis in ((core, kept, keep), (1 - core, given, take)):
        for s in range(half):
            chosen = (row == part) & (col == s)
            w = [jnp.sum(jnp.where(chosen, y, 0.0)) for y in answer]
            slot = len(copies)
            block[slot] = start[s] + (
                w[0] * basis[0, s] + (w[1] * basis[1, s] + w[2] * basis[2, s])
            )
            copy = pltpu.make_async_copy(
                block.at[slot], out.at[part * half + s, 0], done.at[slot]
            )
            copy.start()
            copies.append(copy)
    for copy in copies:
        copy.wait()


def section(state, explicit_rhs, implicit_rhs, implicit_coef):
    count = lax.axis_size("gz")
    species, planes, ny, nx = state.shape
    half = species // 2
    assert planes == 1 and species % 2 == 0 and count % 8 == 0 and half <= STRIDE
    vmem = pl.BlockSpec(memory_space=pltpu.VMEM)
    params = pltpu.CompilerParams(vmem_limit_bytes=24 << 20)
    device = lax.axis_index("gz")
    odd = device % 2 == 1
    chip_odd = device // 2 % 2 == 1

    core = device % 2
    mine = odd != chip_odd

    def move(value, target):
        pairs = []
        for i in range(count):
            chip, side = target(i // 2, i % 2)
            pairs.append((i, chip % (count // 2) * 2 + side))
        return lax.ppermute(value, "gz", pairs)

    def swap(value):
        return move(value, lambda chip, side: (chip, 1 - side))

    def outer(chip, side):
        odd_chip, upper = chip % 2, chip // 2 % 2
        owned = (side ^ odd_chip) == (odd_chip == upper)
        return chip ^ 2 if owned else chip + (2 if upper else -2)

    def piece(array, part):
        return lax.dynamic_slice_in_dim(array, part * half, half)

    section_in = (
        state + explicit_weights[0] * explicit_rhs[0] + explicit_weights[1] * explicit_rhs[1]
    )
    section_in = (
        section_in + implicit_weights[0] * implicit_rhs[0] + implicit_weights[1] * implicit_rhs[1]
    )
    section_in = section_in[:, 0]
    kept, given = lax.optimization_barrier((piece(section_in, core), piece(section_in, 1 - core)))

    def paired(keep, take):
        return jnp.where(mine, take, keep), jnp.where(mine, keep, take)

    next_a = move(kept, lambda chip, side: (chip ^ 1, side))
    outer_a = move(kept, lambda chip, side: (outer(chip, side), side))
    next_b = move(given, lambda chip, side: (chip ^ 1, 1 - side))
    outer_b = move(given, lambda chip, side: (outer(chip, side), 1 - side))
    far = move(kept, lambda chip, side: (chip + (-4 if side else 4), side))
    first, second = paired(kept, swap(given))
    near_x, far_x = paired(next_a, next_b)
    high2, low2 = paired(outer_a, outer_b)
    far_d = move(near_x, lambda chip, side: (chip + (-2 if chip % 2 else 2), side))
    near_d = move(high2, lambda chip, side: (chip ^ 1, side))
    state_kept = piece(state[:, 0], core)
    state_taken = swap(piece(state[:, 0], 1 - core))
    both_state = jnp.stack(paired(state_kept, state_taken))

    def scratch(*lead):
        return pltpu.VMEM(lead + (ny, nx), jnp.float32)

    def shape(*lead):
        return jax.ShapeDtypeStruct(lead + (ny, nx), jnp.float32)

    known, weight = pl.pallas_call(
        upper_kernel,
        in_specs=[vmem] * 7,
        out_specs=[vmem] * 2,
        out_shape=[shape(6, half), shape(2, half)],
        compiler_params=params,
        name="upper",
    )(first, second, near_x, far_x, high2, low2, both_state)
    keep, give, sums = pl.pallas_call(
        moments_kernel,
        in_specs=[vmem] * 9,
        out_specs=[vmem] * 3,
        out_shape=[
            shape(3, half),
            shape(3, half),
            jax.ShapeDtypeStruct((count, 1, 128), jnp.float32),
        ],
        scratch_shapes=[scratch(2), scratch(2), scratch(2), pltpu.VMEM((128, 128), jnp.float32)],
        compiler_params=params,
        name="moments",
    )(first, low2, near_x, far_x, near_d, far_d, far, known, weight)
    parts = lax.all_to_all(sums, "gz", 0, 0)
    take = swap(give)
    coef = jnp.tile(
        jnp.pad(implicit_coef.reshape(2, half), ((0, 0), (0, 128 - half)), constant_values=1.0),
        (4, 1),
    )
    cells = species * count * ny * nx
    value, rms = pl.pallas_call(
        lambda *refs: steps_kernel(*refs, cells=cells),
        in_specs=[vmem] * 6,
        out_specs=[pl.BlockSpec(memory_space=pl.ANY), vmem],
        out_shape=[
            jax.ShapeDtypeStruct(state.shape, jnp.float32),
            jax.ShapeDtypeStruct((1, 1), jnp.float32),
        ],
        scratch_shapes=[scratch(species), pltpu.SemaphoreType.DMA((species,))],
        compiler_params=params,
        name="steps",
    )(parts, coef, kept, given, keep, take)
    return (value, rms[0, 0])


def solution(mesh):
    placed = (
        P(None, "gz", None, None),
        P(None, None, "gz", None, None),
        P(None, None, "gz", None, None),
        P(),
    )
    return jax.shard_map(
        section,
        mesh=mesh,
        in_specs=placed,
        out_specs=(P(None, "gz", None, None), P()),
        check_vma=False,
    )
```

```python
import jax
import jax.numpy as jnp
from jax import lax
from jax.experimental import pallas as pl
from jax.experimental.pallas import tpu as pltpu
from jax.sharding import PartitionSpec as P


explicit_weights = (5535828885825.0 / 10492691773637.0, 788022342437.0 / 10882634858940.0)
implicit_weights = (2746238789719.0 / 10658868560708.0, -640167445237.0 / 6845629431997.0)

STRIDE = 8


def beside_plane(field):
    rows, cols = field.shape
    row = lax.broadcasted_iota(jnp.int32, field.shape, 0)
    col = lax.broadcasted_iota(jnp.int32, field.shape, 1)
    left = jnp.where(col == 0, 0.0, pltpu.roll(field, 1, 1))
    right = jnp.where(col == cols - 1, 0.0, pltpu.roll(field, cols - 1, 1))
    up = jnp.where(row == 0, 0.0, pltpu.roll(field, 1, 0))
    down = jnp.where(row == rows - 1, 0.0, pltpu.roll(field, rows - 1, 0))
    return (left + right) + (up + down)


def half_beside(field):
    row = lax.broadcasted_iota(jnp.int32, field.shape, 0)
    col = lax.broadcasted_iota(jnp.int32, field.shape, 1)
    left = jnp.where(col == 0, 0.0, pltpu.roll(field, 1, 1))
    up = jnp.where(row == 0, 0.0, pltpu.roll(field, 1, 0))
    return left + up


def folded(values):
    rows, cols = values.shape
    total = None
    for r in range(0, rows, 8):
        for c in range(0, cols, 128):
            piece = values[r : r + 8, c : c + 128]
            total = piece if total is None else total + piece
    return total


def upper_kernel(first, second, near_x, far_x, high2, low2, state, all_coef, known, weight, coef):
    half = first.shape[0]
    core = lax.axis_index("gz") % 2
    row = lax.broadcasted_iota(jnp.int32, coef.shape, 0)
    col = lax.broadcasted_iota(jnp.int32, coef.shape, 1)
    column = jnp.zeros(coef.shape, jnp.float32)
    for s in range(half):
        column = jnp.where((row == s) & (col == 0), all_coef[core * half + s], column)
    coef[...] = column

    def species(s, carry):
        b0, b1, b2, b3, b4 = first[s], second[s], near_x[s], far_x[s], high2[s]
        known[2, s] = beside_plane(b0) - 6.0 * b0 + b1
        known[3, s] = beside_plane(low2[s]) - 6.0 * low2[s]
        a1 = beside_plane(b1) - 6.0 * b1 + (b0 + b2)
        known[0, s] = a1
        a2 = beside_plane(b2) - 6.0 * b2 + (b1 + b3)
        known[4, s] = beside_plane(a1) + a2
        a3 = beside_plane(b3) - 6.0 * b3 + (b2 + b4)
        c2 = beside_plane(a2) + (a1 + a3)
        known[1, s] = c2
        a4 = beside_plane(b4) - 6.0 * b4 + b3
        c3 = beside_plane(a3) + (a2 + a4)
        known[5, s] = beside_plane(c2) + c3
        for z in range(2):
            weight[z, s] = 1.0 / (1.0 + 0.1 * jnp.abs(state[z, s]))
        return carry

    lax.fori_loop(0, half, species, 0)


def moments_kernel(
    first, low2, near_x, far_x, near_d, far_d, far, known, weight, coef, keep, give, sums, g0, g1, g2, rows
):
    half = first.shape[0]
    device = lax.axis_index("gz")
    mine = (device + device // 2) % 2
    rows[...] = jnp.zeros(rows.shape, jnp.float32)
    rows[12 * STRIDE : 13 * STRIDE, :] = coef[...]

    def species(s, carry):
        below, below2 = near_d[s], far_d[s]
        under0 = known[2, s] + below
        g0[0] = under0
        g0[1] = known[0, s]
        under1 = beside_plane(below) - 6.0 * below + (first[s] + below2)
        under2 = beside_plane(below2) - 6.0 * below2 + (below + low2[s])
        under3 = known[3, s] + below2
        c2 = beside_plane(under2) + (under1 + under3)
        c1 = beside_plane(under1) + (under0 + under2)
        g1[0] = beside_plane(under0) + (under1 + g0[1])
        g1[1] = known[4, s] + under0
        lower = beside_plane(c1) + (c2 + g1[0])
        g2[0] = beside_plane(g1[0]) + (c1 + g1[1])
        g2[1] = beside_plane(g1[1]) + (g1[0] + known[1, s])
        upper = known[5, s] + g1[1]
        moments = [None] * 12

        def put(k, value):
            value = folded(value)
            moments[k] = value if moments[k] is None else moments[k] + value

        for z in range(2):
            a, b, c = g0[z], g1[z], g2[z]
            put(0, a * a)
            put(1, a * b)
            put(2, b * b)
            put(3, b * c)
            put(4, c * c)
            put(5, c * half_beside(c))
            w = weight[z, s]
            a, b, c = a * w, b * w, c * w
            put(6, a * a)
            put(7, a * b)
            put(8, a * c)
            put(9, b * b)
            put(10, b * c)
            put(11, c * c)
        across = g2[0] * g2[1]
        across = across + 0.5 * (upper * (g2[1] + below2))
        across = across + 0.5 * (lower * (g2[0] + far_x[s]))
        across = across + far[s] * jnp.where(mine == 1, near_x[s], below)
        put(5, across)
        moments[5] = 2.0 * moments[5]
        for k, g in enumerate((g0, g1, g2)):
            keep[k, s] = g[mine]
            give[k, s] = g[1 - mine]
        for k in range(12):
            rows[pl.ds(k * STRIDE + s, 1), :] = jnp.sum(moments[k], axis=0, keepdims=True)
        return carry

    lax.fori_loop(0, half, species, 0)
    summed = jnp.sum(jnp.transpose(rows[...]), axis=0, keepdims=True)
    sums[...] = jnp.broadcast_to(summed[None], sums.shape)


def steps_kernel(parts, kept, given, keep, take, out, rms, block, done, *, cells):
    half = kept.shape[0]
    core = lax.axis_index("gz") % 2
    devices = parts.shape[0]
    total = parts[0:8, 0, :]
    for d in range(8, devices, 8):
        total = total + parts[d : d + 8, 0, :]
    total = total + pltpu.roll(total, 2, 0)
    total = total + pltpu.roll(total, 4, 0)
    m = [total if k == 0 else pltpu.roll(total, 128 - k * STRIDE, 1) for k in range(12)]
    c = pltpu.roll(parts[0:8, 0, :], 128 - 12 * STRIDE, 1)
    diag = 1.0 + 6.0 * c
    smallest = 1.0 / (1.0 + 12.0 * c)

    def inner(p, q, shift):
        result = None
        for i, pi in enumerate(p):
            for j, qj in enumerate(q):
                term = pi * qj * m[i + j + shift]
                result = term if result is None else result + term
        return result

    def times(p):
        zero = jnp.zeros_like(c)
        return [diag * a - c * b for a, b in zip(list(p) + [zero], [zero] + list(p))]

    residual = [jnp.ones_like(c)]
    direction = list(residual)
    norm_now = m[0]
    answer = [jnp.zeros_like(c)] * 3
    for iteration in range(3):
        energy = diag * inner(direction, direction, 0) - c * inner(direction, direction, 1)
        step = jnp.minimum(jnp.maximum(norm_now / energy, smallest), 1.0)
        answer = [a + step * d for a, d in zip(answer, direction + [jnp.zeros_like(c)] * 3)]
        if iteration + 1 < 3:
            image = times(direction)
            residual = [a - step * b for a, b in zip(residual + [jnp.zeros_like(c)], image)]
            norm_next = jnp.maximum(inner(residual, residual, 0), 0.0)
            beta = norm_next / norm_now
            direction = [a + beta * b for a, b in zip(residual, direction + [jnp.zeros_like(c)])]
            norm_now = norm_next
    answer = [c * a for a in answer]
    y0, y1, y2 = answer
    error = (
        y0 * y0 * m[6]
        + y1 * y1 * m[9]
        + y2 * y2 * m[11]
        + 2.0 * (y0 * y1 * m[7] + y0 * y2 * m[8] + y1 * y2 * m[10])
    )
    row = lax.broadcasted_iota(jnp.int32, c.shape, 0)
    col = lax.broadcasted_iota(jnp.int32, c.shape, 1)
    error = jnp.sum(jnp.where((row < 2) & (col < half), error, 0.0), keepdims=True)
    rms[...] = jnp.sqrt(jnp.maximum(error, 0.0) * (1.0 / cells))
    copies = []
    for part, start, basis in ((core, kept, keep), (1 - core, given, take)):
        for s in range(half):
            chosen = (row == part) & (col == s)
            w = [jnp.sum(jnp.where(chosen, y, 0.0)) for y in answer]
            slot = len(copies)
            block[slot] = start[s] + (
                w[0] * basis[0, s] + (w[1] * basis[1, s] + w[2] * basis[2, s])
            )
            copy = pltpu.make_async_copy(
                block.at[slot], out.at[part * half + s, 0], done.at[slot]
            )
            copy.start()
            copies.append(copy)
    for copy in copies:
        copy.wait()


def section(state, explicit_rhs, implicit_rhs, implicit_coef):
    count = lax.axis_size("gz")
    species, planes, ny, nx = state.shape
    half = species // 2
    assert planes == 1 and species % 2 == 0 and count % 8 == 0 and half <= STRIDE
    vmem = pl.BlockSpec(memory_space=pltpu.VMEM)
    params = pltpu.CompilerParams(vmem_limit_bytes=24 << 20)
    device = lax.axis_index("gz")
    odd = device % 2 == 1
    chip_odd = device // 2 % 2 == 1

    core = device % 2
    mine = odd != chip_odd

    def move(value, target):
        pairs = []
        for i in range(count):
            chip, side = target(i // 2, i % 2)
            pairs.append((i, chip % (count // 2) * 2 + side))
        return lax.ppermute(value, "gz", pairs)

    def swap(value):
        return move(value, lambda chip, side: (chip, 1 - side))

    def outer(chip, side):
        odd_chip, upper = chip % 2, chip // 2 % 2
        owned = (side ^ odd_chip) == (odd_chip == upper)
        return chip ^ 2 if owned else chip + (2 if upper else -2)

    def piece(array, part):
        return lax.dynamic_slice_in_dim(array, part * half, half)

    section_in = (
        state + explicit_weights[0] * explicit_rhs[0] + explicit_weights[1] * explicit_rhs[1]
    )
    section_in = (
        section_in + implicit_weights[0] * implicit_rhs[0] + implicit_weights[1] * implicit_rhs[1]
    )
    section_in = section_in[:, 0]
    part_a = jnp.where(mine, core, 1 - core)
    part_a, part_b, kept, given = lax.optimization_barrier(
        tuple(piece(section_in, part) for part in (part_a, 1 - part_a, core, 1 - core))
    )

    def paired(keep, take):
        return jnp.where(mine, take, keep), jnp.where(mine, keep, take)

    def early(chip, side):
        return (chip ^ 1, side) if side ^ chip % 2 else (outer(chip, side), 1 - side)

    def late(chip, side):
        return (outer(chip, side), side) if side ^ chip % 2 else (chip ^ 1, 1 - side)

    def crossed(target):
        return lambda chip, side: (target(chip, side)[0], 1 - target(chip, side)[1])

    early_a = move(part_a, early)
    early_b = move(part_b, crossed(early))
    late_a = move(part_a, late)
    late_b = move(part_b, crossed(late))
    near_x, high2 = paired(early_a, early_b)
    far_x, low2 = paired(late_a, late_b)
    far = move(kept, lambda chip, side: (chip + (-4 if side else 4), side))
    first, second = paired(kept, swap(given))
    far_d = move(near_x, lambda chip, side: (chip + (-2 if chip % 2 else 2), side))
    near_d = move(high2, lambda chip, side: (chip ^ 1, side))
    state_kept = piece(state[:, 0], core)
    state_taken = swap(piece(state[:, 0], 1 - core))
    both_state = jnp.stack(paired(state_kept, state_taken))

    def scratch(*lead):
        return pltpu.VMEM(lead + (ny, nx), jnp.float32)

    def shape(*lead):
        return jax.ShapeDtypeStruct(lead + (ny, nx), jnp.float32)

    known, weight, coef = pl.pallas_call(
        upper_kernel,
        in_specs=[vmem] * 7 + [pl.BlockSpec(memory_space=pltpu.SMEM)],
        out_specs=[vmem] * 3,
        out_shape=[
            shape(6, half),
            shape(2, half),
            jax.ShapeDtypeStruct((STRIDE, 128), jnp.float32),
        ],
        compiler_params=params,
        name="upper",
    )(first, second, near_x, far_x, high2, low2, both_state, implicit_coef)
    keep, give, sums = pl.pallas_call(
        moments_kernel,
        in_specs=[vmem] * 10,
        out_specs=[vmem] * 3,
        out_shape=[
            shape(3, half),
            shape(3, half),
            jax.ShapeDtypeStruct((count, 1, 128), jnp.float32),
        ],
        scratch_shapes=[scratch(2), scratch(2), scratch(2), pltpu.VMEM((128, 128), jnp.float32)],
        compiler_params=params,
        name="moments",
    )(first, low2, near_x, far_x, near_d, far_d, far, known, weight, coef)
    parts = lax.all_to_all(sums, "gz", 0, 0)
    take = swap(give)
    cells = species * count * ny * nx
    value, rms = pl.pallas_call(
        lambda *refs: steps_kernel(*refs, cells=cells),
        in_specs=[vmem] * 5,
        out_specs=[pl.BlockSpec(memory_space=pl.ANY), vmem],
        out_shape=[
            jax.ShapeDtypeStruct(state.shape, jnp.float32),
            jax.ShapeDtypeStruct((1, 1), jnp.float32),
        ],
        scratch_shapes=[scratch(species), pltpu.SemaphoreType.DMA((species,))],
        compiler_params=params,
        name="steps",
    )(parts, kept, given, keep, take)
    return (value, rms[0, 0])


def solution(mesh):
    placed = (
        P(None, "gz", None, None),
        P(None, None, "gz", None, None),
        P(None, None, "gz", None, None),
        P(),
    )
    return jax.shard_map(
        section,
        mesh=mesh,
        in_specs=placed,
        out_specs=(P(None, "gz", None, None), P()),
        check_vma=False,
    )
```

```python
import jax
import jax.numpy as jnp
from jax import lax
from jax.experimental import pallas as pl
from jax.experimental.pallas import tpu as pltpu
from jax.sharding import PartitionSpec as P


explicit_weights = (5535828885825.0 / 10492691773637.0, 788022342437.0 / 10882634858940.0)
implicit_weights = (2746238789719.0 / 10658868560708.0, -640167445237.0 / 6845629431997.0)

GROUP = 1
STRIDE = 8


def beside_plane(field):
    rows, cols = field.shape
    row = lax.broadcasted_iota(jnp.int32, field.shape, 0)
    col = lax.broadcasted_iota(jnp.int32, field.shape, 1)
    left = jnp.where(col == 0, 0.0, pltpu.roll(field, 1, 1))
    right = jnp.where(col == cols - 1, 0.0, pltpu.roll(field, cols - 1, 1))
    up = jnp.where(row == 0, 0.0, pltpu.roll(field, 1, 0))
    down = jnp.where(row == rows - 1, 0.0, pltpu.roll(field, rows - 1, 0))
    return (left + right) + (up + down)


def folded(values):
    rows, cols = values.shape
    total = None
    for r in range(0, rows, 8):
        for c in range(0, cols, 128):
            piece = values[r : r + 8, c : c + 128]
            total = piece if total is None else total + piece
    return total


def upper_kernel(first, second, near_x, far_x, high2, low2, state, all_coef, known, weight, coef):
    half = first.shape[0]
    core = lax.axis_index("gz") % 2
    row = lax.broadcasted_iota(jnp.int32, coef.shape, 0)
    col = lax.broadcasted_iota(jnp.int32, coef.shape, 1)
    column = jnp.zeros(coef.shape, jnp.float32)
    for s in range(half):
        column = jnp.where((row == s) & (col == 0), all_coef[core * half + s], column)
    coef[...] = column

    def species(s, carry):
        b0, b1, b2, b3, b4 = first[s], second[s], near_x[s], far_x[s], high2[s]
        known[2, s] = beside_plane(b0) - 6.0 * b0 + b1
        known[3, s] = beside_plane(low2[s]) - 6.0 * low2[s]
        a1 = beside_plane(b1) - 6.0 * b1 + (b0 + b2)
        known[0, s] = a1
        a2 = beside_plane(b2) - 6.0 * b2 + (b1 + b3)
        known[4, s] = beside_plane(a1) + a2
        a3 = beside_plane(b3) - 6.0 * b3 + (b2 + b4)
        c2 = beside_plane(a2) + (a1 + a3)
        known[1, s] = c2
        a4 = beside_plane(b4) - 6.0 * b4 + b3
        c3 = beside_plane(a3) + (a2 + a4)
        known[5, s] = beside_plane(c2) + c3
        for z in range(2):
            weight[z, s] = 1.0 / (1.0 + 0.1 * jnp.abs(state[z, s]))
        return carry

    lax.fori_loop(0, half, species, 0)


def moments_kernel(
    first, low2, near_x, far_x, near_d, far_d, far, known, weight, coef, keep, give, sums, g0, g1, g2, lower_planes, rows
):
    half, ny, nx = first.shape
    tiles = range(nx // 128)
    device = lax.axis_index("gz")
    mine = (device + device // 2) % 2
    rows[...] = jnp.zeros(rows.shape, jnp.float32)
    rows[12 * STRIDE : 13 * STRIDE, :] = coef[...]
    for planes in (g0, g1, g2, lower_planes):
        edge = jnp.zeros((*planes.shape[:3], 8, 128), jnp.float32)
        planes[:, :, :, 0:8] = edge
        planes[:, :, :, ny + 8 : ny + 16] = edge
    lane = lax.broadcasted_iota(jnp.int32, (ny, 128), 1)

    group = GROUP if half % GROUP == 0 else 1
    pieces = [(q, t) for q in range(group) for t in tiles]
    last = len(tiles) - 1

    def add(*terms):
        return [sum(parts[1:], parts[0]) for parts in zip(*terms)]

    def times(x, y):
        return [u * v for u, v in zip(x, y)]

    def left_of(value):
        rolled = [pltpu.roll(v, 1, 1) for v in value]
        return [
            jnp.where(lane == 0, rolled[i - 1] if t else 0.0, rolled[i])
            for i, (_, t) in enumerate(pieces)
        ]

    def right_of(value):
        rolled = [pltpu.roll(v, 127, 1) for v in value]
        return [
            jnp.where(lane == 127, rolled[i + 1] if t < last else 0.0, rolled[i])
            for i, (_, t) in enumerate(pieces)
        ]

    def store(planes, p, value):
        for (q, t), v in zip(pieces, value):
            planes[p, q, t, 8 : ny + 8] = v

    def load(planes, p, shift=0):
        return [planes[p, q, t, 8 + shift : ny + 8 + shift] for q, t in pieces]

    def beside(planes, p, value):
        return add(
            add(left_of(value), right_of(value)), add(load(planes, p, -1), load(planes, p, 1))
        )

    def some(step, carry):
        s = step * group

        def read(ref, *lead):
            return [ref[(*lead, s + q)][:, t * 128 : (t + 1) * 128] for q, t in pieces]

        below, below2 = read(near_d), read(far_d)
        store(lower_planes, 0, below)
        store(lower_planes, 1, below2)
        under0 = add(read(known, 2), below)
        above = read(known, 0)
        store(g0, 0, under0)
        store(g0, 1, above)
        b1 = add(read(known, 4), under0)
        store(g1, 1, b1)
        upper = add(read(known, 5), b1)
        under1 = add(
            beside(lower_planes, 0, below), [-6.0 * v for v in below], add(read(first), below2)
        )
        store(lower_planes, 2, under1)
        under2 = add(
            beside(lower_planes, 1, below2), [-6.0 * v for v in below2], add(below, read(low2))
        )
        store(lower_planes, 3, under2)
        under3 = add(read(known, 3), below2)
        b0 = add(beside(g0, 0, under0), add(under1, above))
        store(g1, 0, b0)
        c1 = add(beside(lower_planes, 2, under1), add(under0, under2))
        store(lower_planes, 4, c1)
        store(g2, 1, add(beside(g1, 1, b1), add(b0, read(known, 1))))
        c2 = add(beside(lower_planes, 3, under2), add(under1, under3))
        store(g2, 0, add(beside(g1, 0, b0), add(c1, b1)))
        lower = add(beside(lower_planes, 4, c1), add(c2, b0))
        moments = [[None] * 12 for _ in range(group)]

        def put(k, value):
            for (q, _), piece in zip(pieces, value):
                piece = folded(piece)
                moments[q][k] = piece if moments[q][k] is None else moments[q][k] + piece

        for z in (1, 0):
            a, b, c = load(g0, z), load(g1, z), load(g2, z)
            put(5, times(c, add(left_of(c), load(g2, z, -1))))
            put(0, times(a, a))
            put(1, times(a, b))
            put(2, times(b, b))
            put(3, times(b, c))
            put(4, times(c, c))
            w = read(weight, z)
            a, b, c = times(a, w), times(b, w), times(c, w)
            put(6, times(a, a))
            put(7, times(a, b))
            put(8, times(a, c))
            put(9, times(b, b))
            put(10, times(b, c))
            put(11, times(c, c))
        c0, c1 = load(g2, 0), load(g2, 1)
        halves = add(times(upper, add(c1, below2)), times(lower, add(c0, read(far_x))))
        mate = [jnp.where(mine == 1, x, d) for x, d in zip(read(near_x), below)]
        put(5, add(times(c0, c1), [0.5 * v for v in halves], times(read(far), mate)))
        for k, g in enumerate((g0, g1, g2)):
            for q, t in pieces:
                cut = slice(t * 128, (t + 1) * 128)
                keep[k, s + q, :, cut] = g[mine, q, t, 8 : ny + 8]
                give[k, s + q, :, cut] = g[1 - mine, q, t, 8 : ny + 8]
        for q in range(group):
            moments[q][5] = 2.0 * moments[q][5]
            for k in range(12):
                rows[pl.ds(k * STRIDE + s + q, 1), :] = jnp.sum(
                    moments[q][k], axis=0, keepdims=True
                )
        return carry

    lax.fori_loop(0, half // group, some, 0)
    summed = jnp.sum(jnp.transpose(rows[...]), axis=0, keepdims=True)
    sums[...] = jnp.broadcast_to(summed[None], sums.shape)


def steps_kernel(parts, kept, given, keep, take, out, rms, block, done, *, cells):
    half = kept.shape[0]
    core = lax.axis_index("gz") % 2
    devices = parts.shape[0]
    total = parts[0:8, 0, :]
    for d in range(8, devices, 8):
        total = total + parts[d : d + 8, 0, :]
    total = total + pltpu.roll(total, 2, 0)
    total = total + pltpu.roll(total, 4, 0)
    m = [total if k == 0 else pltpu.roll(total, 128 - k * STRIDE, 1) for k in range(12)]
    c = pltpu.roll(parts[0:8, 0, :], 128 - 12 * STRIDE, 1)
    diag = 1.0 + 6.0 * c
    smallest = 1.0 / (1.0 + 12.0 * c)

    def inner(p, q, shift):
        result = None
        for i, pi in enumerate(p):
            for j, qj in enumerate(q):
                term = pi * qj * m[i + j + shift]
                result = term if result is None else result + term
        return result

    def times(p):
        zero = jnp.zeros_like(c)
        return [diag * a - c * b for a, b in zip(list(p) + [zero], [zero] + list(p))]

    residual = [jnp.ones_like(c)]
    direction = list(residual)
    norm_now = m[0]
    answer = [jnp.zeros_like(c)] * 3
    for iteration in range(3):
        energy = diag * inner(direction, direction, 0) - c * inner(direction, direction, 1)
        step = jnp.minimum(jnp.maximum(norm_now / energy, smallest), 1.0)
        answer = [a + step * d for a, d in zip(answer, direction + [jnp.zeros_like(c)] * 3)]
        if iteration + 1 < 3:
            image = times(direction)
            residual = [a - step * b for a, b in zip(residual + [jnp.zeros_like(c)], image)]
            norm_next = jnp.maximum(inner(residual, residual, 0), 0.0)
            beta = norm_next / norm_now
            direction = [a + beta * b for a, b in zip(residual, direction + [jnp.zeros_like(c)])]
            norm_now = norm_next
    answer = [c * a for a in answer]
    y0, y1, y2 = answer
    error = (
        y0 * y0 * m[6]
        + y1 * y1 * m[9]
        + y2 * y2 * m[11]
        + 2.0 * (y0 * y1 * m[7] + y0 * y2 * m[8] + y1 * y2 * m[10])
    )
    row = lax.broadcasted_iota(jnp.int32, c.shape, 0)
    col = lax.broadcasted_iota(jnp.int32, c.shape, 1)
    error = jnp.sum(jnp.where((row < 2) & (col < half), error, 0.0), keepdims=True)
    rms[...] = jnp.sqrt(jnp.maximum(error, 0.0) * (1.0 / cells))
    copies = []
    for part, start, basis in ((core, kept, keep), (1 - core, given, take)):
        for s in range(half):
            chosen = (row == part) & (col == s)
            w = [jnp.sum(jnp.where(chosen, y, 0.0)) for y in answer]
            slot = len(copies)
            block[slot] = start[s] + (
                w[0] * basis[0, s] + (w[1] * basis[1, s] + w[2] * basis[2, s])
            )
            copy = pltpu.make_async_copy(
                block.at[slot], out.at[part * half + s, 0], done.at[slot]
            )
            copy.start()
            copies.append(copy)
    for copy in copies:
        copy.wait()


def section(state, explicit_rhs, implicit_rhs, implicit_coef):
    count = lax.axis_size("gz")
    species, planes, ny, nx = state.shape
    half = species // 2
    assert planes == 1 and species % 2 == 0 and count % 8 == 0 and half <= STRIDE
    vmem = pl.BlockSpec(memory_space=pltpu.VMEM)
    params = pltpu.CompilerParams(vmem_limit_bytes=24 << 20)
    device = lax.axis_index("gz")
    odd = device % 2 == 1
    chip_odd = device // 2 % 2 == 1

    core = device % 2
    mine = odd != chip_odd

    def move(value, target):
        pairs = []
        for i in range(count):
            chip, side = target(i // 2, i % 2)
            pairs.append((i, chip % (count // 2) * 2 + side))
        return lax.ppermute(value, "gz", pairs)

    def swap(value):
        return move(value, lambda chip, side: (chip, 1 - side))

    def outer(chip, side):
        odd_chip, upper = chip % 2, chip // 2 % 2
        owned = (side ^ odd_chip) == (odd_chip == upper)
        return chip ^ 2 if owned else chip + (2 if upper else -2)

    def piece(array, part):
        return lax.dynamic_slice_in_dim(array, part * half, half)

    section_in = (
        state + explicit_weights[0] * explicit_rhs[0] + explicit_weights[1] * explicit_rhs[1]
    )
    section_in = (
        section_in + implicit_weights[0] * implicit_rhs[0] + implicit_weights[1] * implicit_rhs[1]
    )
    section_in = section_in[:, 0]
    part_a = jnp.where(mine, core, 1 - core)
    part_a, part_b, kept, given = lax.optimization_barrier(
        tuple(piece(section_in, part) for part in (part_a, 1 - part_a, core, 1 - core))
    )

    def paired(keep, take):
        return jnp.where(mine, take, keep), jnp.where(mine, keep, take)

    def early(chip, side):
        return (chip ^ 1, side) if side ^ chip % 2 else (outer(chip, side), 1 - side)

    def late(chip, side):
        return (outer(chip, side), side) if side ^ chip % 2 else (chip ^ 1, 1 - side)

    def crossed(target):
        return lambda chip, side: (target(chip, side)[0], 1 - target(chip, side)[1])

    early_a = move(part_a, early)
    early_b = move(part_b, crossed(early))
    late_a = move(part_a, late)
    late_b = move(part_b, crossed(late))
    near_x, high2 = paired(early_a, early_b)
    far_x, low2 = paired(late_a, late_b)
    far = move(kept, lambda chip, side: (chip + (-4 if side else 4), side))
    first, second = paired(kept, swap(given))
    far_d = move(near_x, lambda chip, side: (chip + (-2 if chip % 2 else 2), side))
    near_d = move(high2, lambda chip, side: (chip ^ 1, side))
    state_kept = piece(state[:, 0], core)
    state_taken = swap(piece(state[:, 0], 1 - core))
    both_state = jnp.stack(paired(state_kept, state_taken))

    def scratch(*lead):
        return pltpu.VMEM(lead + (ny, nx), jnp.float32)

    def shape(*lead):
        return jax.ShapeDtypeStruct(lead + (ny, nx), jnp.float32)

    known, weight, coef = pl.pallas_call(
        upper_kernel,
        in_specs=[vmem] * 7 + [pl.BlockSpec(memory_space=pltpu.SMEM)],
        out_specs=[vmem] * 3,
        out_shape=[
            shape(6, half),
            shape(2, half),
            jax.ShapeDtypeStruct((STRIDE, 128), jnp.float32),
        ],
        compiler_params=params,
        name="upper",
    )(first, second, near_x, far_x, high2, low2, both_state, implicit_coef)
    keep, give, sums = pl.pallas_call(
        moments_kernel,
        in_specs=[vmem] * 10,
        out_specs=[vmem] * 3,
        out_shape=[
            shape(3, half),
            shape(3, half),
            jax.ShapeDtypeStruct((count, 1, 128), jnp.float32),
        ],
        scratch_shapes=[
            pltpu.VMEM((planes, GROUP, nx // 128, ny + 16, 128), jnp.float32)
            for planes in (2, 2, 2, 5)
        ]
        + [pltpu.VMEM((128, 128), jnp.float32)],
        compiler_params=params,
        name="moments",
    )(first, low2, near_x, far_x, near_d, far_d, far, known, weight, coef)
    parts = lax.all_to_all(sums, "gz", 0, 0)
    take = swap(give)
    cells = species * count * ny * nx
    value, rms = pl.pallas_call(
        lambda *refs: steps_kernel(*refs, cells=cells),
        in_specs=[vmem] * 5,
        out_specs=[pl.BlockSpec(memory_space=pl.ANY), vmem],
        out_shape=[
            jax.ShapeDtypeStruct(state.shape, jnp.float32),
            jax.ShapeDtypeStruct((1, 1), jnp.float32),
        ],
        scratch_shapes=[scratch(species), pltpu.SemaphoreType.DMA((species,))],
        compiler_params=params,
        name="steps",
    )(parts, kept, given, keep, take)
    return (value, rms[0, 0])


def solution(mesh):
    placed = (
        P(None, "gz", None, None),
        P(None, None, "gz", None, None),
        P(None, None, "gz", None, None),
        P(),
    )
    return jax.shard_map(
        section,
        mesh=mesh,
        in_specs=placed,
        out_specs=(P(None, "gz", None, None), P()),
        check_vma=False,
    )
```
